256 devices in a mesh: group: 8 (over z_hi, y), shard: 32 (over x, z_lo, core).
Axes of the slice: x: 4, y: 4, z: 8 (z_hi: 2, z_lo: 4; z = z_hi * 4 + z_lo), core: 2. Of those that a mesh axis runs over, the one named last changes fastest.
Arguments:
- gradients: bfloat16 [8, 32, 256, 8192], P('group', 'shard'), may hold values from -1.59375 to 1.59375
- momentum: float32 [8, 256, 8192], P('group', None, 'shard'), may hold values from -6 to 6
- master: float32 [256, 8192], P(None, 'shard'), may hold values from -0.6 to 0.6
- indices: int32 [8, 4, 128, 32], P('group', None, 'shard'), may hold values from 0 to 4095, as said below
Outputs:
- momentum_out: float32 [8, 256, 8192], P('group', None, 'shard')
- master_out: float32 [256, 8192], P(None, 'shard')
- params_full: bfloat16 [256, 8192], replicated
The draws below stay inside these ranges and needn't reach their ends.
Inputs may be any that keep to these rules, and one draw needn't show every extreme that they name: `indices`: the 32 positions of one group and block are distinct.
All inputs are finite; a program needn't handle non-finite values.
Results may differ from the reference program's by a relative error of at most 0.001.
Values may be sent and summed in bfloat16 or wider, within the bound.
No kernel may reach another device: no remote copies, remote signals or barrier semaphores. Data moves between devices by JAX's collectives and lax.ppermute only.
A program may use at most 128 MiB of HBM per device.

```python
import jax
import jax.numpy as jnp
from jax import lax

D = 8192
ROWS = 256
BLOCK = 64
TOPK = 32
N_GROUP = 8
N_SHARD = 32


def draw_indices(key, part):
    scores = jax.random.randint(key, (N_GROUP, ROWS // BLOCK, D // BLOCK, BLOCK * BLOCK), 0, 2 ** 18)
    scores = scores * (BLOCK * BLOCK) + lax.broadcasted_iota(jnp.int32, scores.shape, 3)
    return lax.top_k(scores, TOPK)[1].astype(jnp.int32)


def strengthened(entries, stream_key, source, target, blocks, factor):
    def block_of(position):
        return (jnp.arange(entries.shape[position]) // (entries.shape[position] // blocks)).reshape((-1,) + (1,) * (entries.ndim - 1 - position))

    near = jax.random.permutation(stream_key, blocks)[block_of(target)]
    far = (block_of(target) + blocks // 2) % blocks
    return jnp.where((block_of(source) == near) | (block_of(source) == far), factor * entries, entries)


def levels(rng, dims, split, smallest, top_value):
    def one(position, blocks):
        draws = jax.random.uniform(jax.random.fold_in(jax.random.fold_in(rng, 6), position), (blocks,), jnp.float32, smallest / len(split), top_value / len(split))
        return jnp.repeat(jnp.exp(draws), dims[position] // blocks).reshape((-1,) + (1,) * (len(dims) - position - 1))

    level = one(*split[0])
    for cut in split[1:]:
        level = level * one(*cut)
    return level


def bell_draw(own_key, shape, deviation, bound, shards=(), kind=jnp.bfloat16):
    values = deviation * jax.random.normal(own_key, shape, jnp.float32)
    if shards:
        values = values * levels(own_key, shape, shards, -0.22, 0.18)
    return jnp.clip(values, -bound, bound).astype(kind)


def heavy_noise(key, dims, width, most, shards, heavy, kind=jnp.bfloat16):
    entries = width * jax.random.normal(key, dims, jnp.float32)
    if shards:
        entries = entries * levels(key, dims, shards, -0.22, 0.18)
    return jnp.clip(strengthened(entries, jax.random.fold_in(key, 3), *heavy), -most, most).astype(kind)


def setup_inputs(seed: int = 0) -> dict:
    keys = jax.random.split(jax.random.key(seed), 5)
    return {
        "gradients": heavy_noise(keys[0], (N_GROUP, N_SHARD, ROWS, D), 0.2, 1.59375, ((0, 8), (1, 32)), (1, 3, 32, 2.75)),
        "momentum": bell_draw(keys[1], (N_GROUP, ROWS, D), 1.0, 6.0, ((0, 8), (2, 32)), jnp.float32),
        "master": bell_draw(keys[2], (ROWS, D), 0.1, 0.6, ((1, 32),), jnp.float32),
        "indices": draw_indices(jax.random.fold_in(keys[4], 71), 0),
    }


momentum_decay = 0.9
step_rate = 0.5

def cosine_table(side):
    freqs = jnp.arange(side, dtype=jnp.float32)[:, None]
    places = jnp.arange(side, dtype=jnp.float32)[None, :]
    table = jnp.cos(jnp.pi * (2.0 * places + 1.0) * freqs / (2.0 * side))
    weights = jnp.where(freqs == 0.0, jnp.sqrt(1.0 / side), jnp.sqrt(2.0 / side))
    return table * weights

def into_blocks(field, side):
    leading = field.shape[:-2]
    depth = len(leading)
    shaped = field.reshape(leading + (field.shape[-2] // side, side, field.shape[-1] // side, side))
    return jnp.moveaxis(shaped, depth + 2, depth + 1)

def out_blocks(blocks):
    leading = blocks.shape[:-4]
    depth = len(leading)
    moved = jnp.moveaxis(blocks, depth + 1, depth + 2)
    return moved.reshape(leading + (blocks.shape[-4] * blocks.shape[-2], blocks.shape[-3] * blocks.shape[-1]))

def forward_blocks(blocks, table):
    return jnp.einsum('kn,...nm,lm->...kl', table, blocks, table, precision=lax.Precision.HIGHEST)

def inverse_blocks(blocks, table):
    return jnp.einsum('kn,...kl,lm->...nm', table, blocks, table, precision=lax.Precision.HIGHEST)

def scatter_picked(picked, positions, target_shape):
    places = [lax.broadcasted_iota(jnp.int32, positions.shape, dimension) for dimension in range(positions.ndim - 1)]
    return jnp.zeros(target_shape, picked.dtype).at[tuple(places) + (positions,)].add(picked)

def reference(gradients, momentum, master, indices):
    table = cosine_table(BLOCK)

    def add_device(device_index, running):
        piece = lax.dynamic_index_in_dim(gradients, device_index, 1, keepdims=False)
        return running + piece.astype(jnp.float32)
    summed = lax.fori_loop(0, N_SHARD, add_device, jnp.zeros((N_GROUP, ROWS, D), jnp.float32))
    accumulated = momentum_decay * momentum + summed
    coeffs = forward_blocks(into_blocks(accumulated, BLOCK), table)
    flat = coeffs.reshape(coeffs.shape[:-2] + (BLOCK * BLOCK,))
    picked = jnp.take_along_axis(flat, indices, axis=3)
    own_dense = scatter_picked(picked, indices, flat.shape)
    union_sum = lax.optimization_barrier(jnp.sum(own_dense, axis=0))
    own_field = out_blocks(inverse_blocks(own_dense.reshape(coeffs.shape), table))
    momentum_out = accumulated - own_field
    change_field = out_blocks(inverse_blocks(union_sum.reshape(coeffs.shape[1:]), table))
    master_out = master - step_rate * jnp.tanh(change_field)
    return (momentum_out, master_out, master_out.astype(jnp.bfloat16))
```

```python
import jax
import jax.numpy as jnp
import numpy as np
from jax import lax
from jax.experimental import pallas as pl
from jax.experimental.pallas import tpu as pltpu
from jax.sharding import Mesh
from jax.sharding import PartitionSpec as P


BLOCK = 64
W = 256
SHARD = ("x", "z", "c")
DECAY = 0.9
STEP = 0.5
TOP = 32767.0
PAIR_BOUND = 3.2
OCTET_BOUND = 12.8
HI = lax.Precision.HIGHEST


def cosine_blocks():
    k = np.arange(BLOCK, dtype=np.float64)[:, None]
    n = np.arange(BLOCK, dtype=np.float64)[None, :]
    table = np.cos(np.pi * (2 * n + 1) * k / (2 * BLOCK)) * np.where(k == 0, np.sqrt(1 / BLOCK), np.sqrt(2 / BLOCK))
    return np.kron(np.eye(W // BLOCK), table).astype(np.float32)


def swapped(value, axis, mask):
    size = lax.axis_size(axis)
    return lax.ppermute(value, axis, [(i, i ^ mask) for i in range(size)])


def encode(field, bound):
    top = jnp.max(jnp.abs(field), axis=0, keepdims=True)
    scale = jnp.clip(jnp.ceil(top * (TOP / bound)), 1.0, TOP)
    code = jnp.round(field * ((TOP * TOP / bound) / scale))
    return code.astype(jnp.int32).astype(jnp.int16), jnp.broadcast_to(scale, (16, field.shape[1])).astype(jnp.int32).astype(jnp.int16)


def decode(code, scale, bound):
    return code.astype(jnp.int32).astype(jnp.float32) * (scale.astype(jnp.int32).astype(jnp.float32) * (bound / (TOP * TOP)))


ANY = pl.BlockSpec(memory_space=pl.ANY)
VM = pl.BlockSpec(memory_space=pltpu.VMEM)
HB = pl.BlockSpec(memory_space=pltpu.HBM)
MIB = 1 << 20


def params(mib):
    return pltpu.CompilerParams(vmem_limit_bytes=mib * MIB)


def own_place():
    return [lax.axis_index(name) for name in ("x", "z", "c")]


def column(d, e, flip, place):
    return pl.multiple_of((((place[0] ^ d) * 4 + (place[1] ^ e)) * 2 + (place[2] ^ flip)) * W, W)


def pick_out(grad, zs, after=()):
    n = 4 * len(zs)

    def body(g, *refs):
        out, sem = refs[-2:]
        place = own_place()
        copies = []
        for d in range(4):
            for i, e in enumerate(zs):
                at = d * len(zs) + i
                copy = pltpu.make_async_copy(g.at[:, pl.ds(column(d, e, 1, place), W)], out.at[:, pl.ds(at * W, W)], sem.at[at])
                copy.start()
                copies.append(copy)
        for copy in copies:
            copy.wait()

    return pl.pallas_call(
        body,
        out_shape=jax.ShapeDtypeStruct((W, n * W), jnp.bfloat16),
        in_specs=[HB] + [ANY] * len(after),
        out_specs=VM,
        scratch_shapes=[pltpu.SemaphoreType.DMA((n,))],
        compiler_params=params(8),
        name="pick_out",
    )(grad, *after)


def pair_sums(grad, other, zs, after=()):
    m = len(zs)

    def body(g, o, *refs):
        own, c1, c2, c3, buf, sem = refs[-6:]
        place = own_place()
        gets = {}
        order = (1, 2, 3, 0)
        for d in order:
            for i, e in enumerate(zs):
                n = d * m + i
                gets[n] = pltpu.make_async_copy(g.at[:, pl.ds(column(d, e, 0, place), W)], buf.at[:, pl.ds(n * W, W)], sem.at[n])
                gets[n].start()
        for d in order:
            for i in range(m):
                gets[d * m + i].wait()
                at = pl.ds((d * m + i) * W, W)
                total = buf[:, at].astype(jnp.float32) + o[:, at].astype(jnp.float32)
                to = pl.ds(i * W, W)
                if d == 0:
                    own[:, to] = total
                else:
                    ref = (c1, c2, c3)[d - 1]
                    code, scale = encode(total, PAIR_BOUND)
                    ref[0:W, to] = code
                    ref[W : W + 16, to] = scale

    sent = jax.ShapeDtypeStruct((W + 16, m * W), jnp.int16)
    return pl.pallas_call(
        body,
        out_shape=(jax.ShapeDtypeStruct((W, m * W), jnp.float32), sent, sent, sent),
        in_specs=[HB, VM] + [ANY] * len(after),
        out_specs=(VM, VM, VM, VM),
        scratch_shapes=[pltpu.VMEM((W, 4 * m * W), jnp.bfloat16), pltpu.SemaphoreType.DMA((4 * m,))],
        compiler_params=params(12),
        name="pair_sums",
    )(grad, other, *after)


def octet_sums(own, got, kept, after=()):
    m = own.shape[1] // W

    def body(own, g1, g2, g3, *refs):
        outs = refs[-m:]
        for i in range(m):
            at = pl.ds(i * W, W)
            total = own[:, at]
            for ref in (g1, g2, g3):
                total = total + decode(ref[0:W, at], ref[W : W + 1, at], PAIR_BOUND)
            if i in kept:
                outs[i][...] = total
            else:
                code, scale = encode(total, OCTET_BOUND)
                outs[i][0:W, :] = code
                outs[i][W : W + 16, :] = scale

    shapes = tuple(
        jax.ShapeDtypeStruct((W, W), jnp.float32) if i in kept else jax.ShapeDtypeStruct((W + 16, W), jnp.int16) for i in range(m)
    )
    return pl.pallas_call(
        body,
        out_shape=shapes,
        in_specs=[VM] * 4 + [ANY] * len(after),
        out_specs=tuple(VM for _ in shapes),
        compiler_params=params(12),
        name="octet_sums",
    )(own, *got, *after)


def dot(a, b, dims=((1,), (0,)), precision=None):
    return lax.dot_general(a, b, (dims, ((), ())), precision=precision, preferred_element_type=jnp.float32)


def thirds(value):
    first = value.astype(jnp.bfloat16)
    rest = value - first.astype(jnp.float32)
    second = rest.astype(jnp.bfloat16)
    third = (rest - second.astype(jnp.float32)).astype(jnp.bfloat16)
    return first, second, third


def own_masks(ids):
    lane = lax.broadcasted_iota(jnp.int32, (1, 512), 1)
    down = lax.broadcasted_iota(jnp.int32, (W, 512), 0)
    row = (lane >> 7) * BLOCK + (ids >> 6)
    col = ((lane >> 5) & 3) * BLOCK + (ids & 63)
    return down == row, down == col


def transform(own, got, momentum, table, ids):
    def body(own, g1, g2, g3, mom, table, ids, acc_out, coeff_out, note_out):
        total = own[...]
        for ref in (g1, g2, g3):
            total = total + decode(ref[0:W, :], ref[W : W + 1, :], OCTET_BOUND)
        acc = DECAY * mom[...] + total
        acc_out[...] = acc
        t = table[...]
        coeffs = dot(dot(t, acc, precision=HI), t, ((1,), (1,)), HI)
        coeff_out[...] = coeffs
        rows, cols = own_masks(ids[...])
        chosen = cols.astype(jnp.float32).astype(jnp.bfloat16)
        parts = thirds(coeffs)
        spread = dot(parts[0], chosen) + (dot(parts[1], chosen) + dot(parts[2], chosen))
        note_out[:, 0:512] = jnp.sum(jnp.where(rows, spread, 0.0), axis=0, keepdims=True)
        note_out[:, 512:1024] = ids[...].astype(jnp.float32)

    return pl.pallas_call(
        body,
        out_shape=(
            jax.ShapeDtypeStruct((W, W), jnp.float32),
            jax.ShapeDtypeStruct((W, W), jnp.float32),
            jax.ShapeDtypeStruct((1, 1024), jnp.float32),
        ),
        in_specs=[VM] * 7,
        out_specs=(VM, VM, VM),
        compiler_params=params(16),
        name="transform",
    )(own, *got, momentum, table, ids)


def momentum_step(acc, coeffs, table, ids):
    def body(acc, coeffs, table, ids, out):
        rows, cols = own_masks(ids[...])
        mask = dot(rows.astype(jnp.float32).astype(jnp.bfloat16), cols.astype(jnp.float32).astype(jnp.bfloat16), ((1,), (1,)))
        dense = jnp.where(mask > 0.5, coeffs[...], 0.0)
        t = table[...]
        out[...] = acc[...] - dot(dot(t, dense, ((0,), (0,)), HI), t, precision=HI)

    return pl.pallas_call(
        body,
        out_shape=jax.ShapeDtypeStruct((W, W), jnp.float32),
        in_specs=[VM] * 4,
        out_specs=VM,
        compiler_params=params(16),
        cost_estimate=pl.CostEstimate(flops=10**9, transcendentals=0, bytes_accessed=10**6),
        name="momentum_step",
    )(acc, coeffs, table, ids)


def bundle(parts, after=(), flat=False):
    shape = parts[0].shape
    out_shape = (len(parts),) + (shape[1:] if flat else shape)

    def body(*refs):
        out = refs[-1]
        for i in range(len(parts)):
            if flat:
                out[i : i + 1, :] = refs[i][...]
            else:
                out[i] = refs[i][...]

    return pl.pallas_call(
        body,
        out_shape=jax.ShapeDtypeStruct(out_shape, parts[0].dtype),
        in_specs=[VM] * len(parts) + [HB if flat else ANY] * len(after),
        out_specs=VM,
        compiler_params=params(8),
        name="bundle",
    )(*parts, *after)


def master_step(master, table, near, far):
    def body(master, table, near, far, out, low):
        me = lax.axis_index("group")
        notes = [near[i : i + 1, :] for i in range(4)] + [far[i : i + 1, :] for i in range(4)]
        ordered = []
        for g in range(8):
            rel = me ^ g
            found = notes[0]
            for r in range(1, 8):
                found = jnp.where(rel == r, notes[r], found)
            ordered.append(found)
        bands = []
        for a in range(4):
            v = jnp.concatenate([x[:, a * 128 : a * 128 + 128] for x in ordered], axis=1)
            k = jnp.concatenate([x[:, 512 + a * 128 : 640 + a * 128] for x in ordered], axis=1).astype(jnp.int32)
            lane = lax.broadcasted_iota(jnp.int32, (1, 1024), 1)
            row = lax.broadcasted_iota(jnp.int32, (BLOCK, 1024), 0) == (k >> 6)
            col = lax.broadcasted_iota(jnp.int32, (W, 1024), 0) == (((lane >> 5) & 3) * BLOCK + (k & 63))
            col = col.astype(jnp.float32).astype(jnp.bfloat16)
            stack = jnp.concatenate([jnp.where(row, p.astype(jnp.float32), 0.0).astype(jnp.bfloat16) for p in thirds(v)], axis=0)
            both = dot(stack, col, ((1,), (1,)))
            bands.append(both[0:BLOCK] + (both[BLOCK : 2 * BLOCK] + both[2 * BLOCK :]))
        union = jnp.concatenate(bands, axis=0)
        t = table[...]
        change = dot(dot(t, union, ((0,), (0,)), HI), t, precision=HI)
        result = master[...] - STEP * jnp.tanh(change)
        out[...] = result
        low[...] = result.astype(jnp.bfloat16)

    return pl.pallas_call(
        body,
        out_shape=(jax.ShapeDtypeStruct((W, W), jnp.float32), jax.ShapeDtypeStruct((W, W), jnp.bfloat16)),
        in_specs=[VM] * 4,
        out_specs=(VM, VM),
        compiler_params=params(16),
        name="master_step",
    )(master, table, near, far)


def joined(stacks, keys, whole=None):
    count = sum(len(k) for k in keys)

    def body(*refs):
        out, sem = refs[-2:]
        place = own_place()
        copies = []
        for ref, places in zip(refs, keys):
            for i, key in enumerate(places):
                copy = pltpu.make_async_copy(ref.at[i], out.at[:, pl.ds(column(*key, place), W)], sem.at[len(copies)])
                copy.start()
                copies.append(copy)
        for copy in copies:
            copy.wait()

    more = () if whole is None else (whole,)
    return pl.pallas_call(
        body,
        out_shape=jax.ShapeDtypeStruct((W, 32 * W), jnp.bfloat16),
        in_specs=[VM] * len(stacks) + [ANY] * len(more),
        out_specs=ANY,
        input_output_aliases={len(stacks): 0} if more else {},
        scratch_shapes=[pltpu.SemaphoreType.DMA((count,))],
        compiler_params=params(12),
        name="joined",
    )(*stacks, *more)


def local(gradients, momentum, master, indices):
    table = jnp.asarray(cosine_blocks())
    grad = gradients[0, 0]
    ids = indices[0].reshape(1, 512)

    far, near = (2, 3), (0, 1)
    given_far = pick_out(grad, far)
    given_near = pick_out(grad, near, (given_far,))
    own_far, *codes_far = pair_sums(grad, swapped(given_far, "c", 1), far)
    got_far = [swapped(code, "x", d) for d, code in zip((1, 2, 3), codes_far)]
    own_near, *codes_near = pair_sums(grad, swapped(given_near, "c", 1), near, (own_far,))
    got_near = [swapped(code, "x", d) for d, code in zip((1, 2, 3), codes_near)]
    out2, out3 = octet_sums(own_far, got_far, ())
    in2, in3 = swapped(out2, "z", 2), swapped(out3, "z", 3)
    own, out1 = octet_sums(own_near, got_near, (0,), (out2,))
    in1 = swapped(out1, "z", 1)

    acc, coeffs, note = transform(own, (in1, in2, in3), momentum[0], table, ids)
    notes = [note] + [lax.ppermute(note, "group", [(i, i ^ r) for i in range(8)]) for r in (1, 2, 3)]
    momentum_out = momentum_step(acc, coeffs, table, ids)
    mine = bundle(notes, (momentum_out,), flat=True)
    theirs = lax.ppermute(mine, "group", [(i, i ^ 4) for i in range(8)])
    master_out, low = master_step(master, table, mine, theirs)

    by_z = [low] + [swapped(low, "z", e) for e in (1, 2, 3)]
    by_x = {(d, e): swapped(by_z[e], "x", d) for e in (0, 1) for d in (1, 2, 3)}
    last = bundle(by_z[2:])
    by_x_last = [swapped(last, "x", d) for d in (1, 2, 3)]
    first = bundle(by_z + [by_x[key] for key in by_x], (last,))
    keys = [(0, e) for e in range(4)] + list(by_x)
    whole = joined(
        [first, swapped(first, "c", 1)],
        [[(*key, 0) for key in keys], [(*key, 1) for key in keys]],
    )
    params_full = joined(
        by_x_last + [swapped(part, "c", 1) for part in by_x_last],
        [[(d, 2, f), (d, 3, f)] for f in (0, 1) for d in (1, 2, 3)],
        whole,
    )
    return momentum_out[None], master_out, params_full


def solution(mesh):
    torus = Mesh(mesh.devices.reshape(mesh.shape["group"], 4, 4, 2), ("group", "x", "z", "c"))
    return jax.shard_map(
        local,
        mesh=torus,
        in_specs=(P("group", SHARD, None, None), P("group", None, SHARD), P(None, SHARD), P("group", None, SHARD, None)),
        out_specs=(P("group", None, SHARD), P(None, SHARD), P()),
        check_vma=False,
    )
```

```python
import jax
import jax.numpy as jnp
import numpy as np
from jax import lax
from jax.experimental import pallas as pl
from jax.experimental.pallas import tpu as pltpu
from jax.sharding import Mesh
from jax.sharding import PartitionSpec as P


BLOCK = 64
W = 256
SHARD = ("x", "z", "c")
DECAY = 0.9
STEP = 0.5
TOP = 32767.0
EXTRA = 8
PAIR_BOUND = 3.2
OCTET_BOUND = 12.8
HI = lax.Precision.HIGHEST


def cosine_blocks():
    k = np.arange(BLOCK, dtype=np.float64)[:, None]
    n = np.arange(BLOCK, dtype=np.float64)[None, :]
    table = np.cos(np.pi * (2 * n + 1) * k / (2 * BLOCK)) * np.where(k == 0, np.sqrt(1 / BLOCK), np.sqrt(2 / BLOCK))
    return np.kron(np.eye(W // BLOCK), table).astype(np.float32)


def swapped(value, axis, mask):
    size = lax.axis_size(axis)
    return lax.ppermute(value, axis, [(i, i ^ mask) for i in range(size)])


def encode(field, bound):
    top = jnp.max(jnp.abs(field), axis=0, keepdims=True)
    scale = jnp.clip(jnp.ceil(top * (TOP / bound)), 1.0, TOP)
    code = jnp.round(field * ((TOP * TOP / bound) / scale))
    return code.astype(jnp.int32).astype(jnp.int16), jnp.broadcast_to(scale, (EXTRA, field.shape[1])).astype(jnp.int32).astype(jnp.int16)


def decode(code, scale, bound):
    return code.astype(jnp.int32).astype(jnp.float32) * (scale.astype(jnp.int32).astype(jnp.float32) * (bound / (TOP * TOP)))


ANY = pl.BlockSpec(memory_space=pl.ANY)
VM = pl.BlockSpec(memory_space=pltpu.VMEM)
HB = pl.BlockSpec(memory_space=pltpu.HBM)
MIB = 1 << 20


def params(mib):
    return pltpu.CompilerParams(vmem_limit_bytes=mib * MIB)


def own_place():
    return [lax.axis_index(name) for name in ("x", "z", "c")]


def column(d, e, flip, place):
    return pl.multiple_of((((place[0] ^ d) * 4 + (place[1] ^ e)) * 2 + (place[2] ^ flip)) * W, W)


def pick_out(grad, wanted, after=()):
    def body(g, *refs):
        outs, sem = refs[len(after) : -1], refs[-1]
        place = own_place()
        copies = []
        for out, (zs, flip) in zip(outs, wanted):
            for d in range(4):
                for i, e in enumerate(zs):
                    to = pl.ds((d * len(zs) + i) * W, W)
                    copy = pltpu.make_async_copy(g.at[:, pl.ds(column(d, e, flip, place), W)], out.at[:, to], sem.at[len(copies)])
                    copy.start()
                    copies.append(copy)
        for copy in copies:
            copy.wait()

    return pl.pallas_call(
        body,
        out_shape=tuple(jax.ShapeDtypeStruct((W, 4 * len(zs) * W), jnp.bfloat16) for zs, _ in wanted),
        in_specs=[HB] + [ANY] * len(after),
        out_specs=(VM,) * len(wanted),
        scratch_shapes=[pltpu.SemaphoreType.DMA((4 * sum(len(zs) for zs, _ in wanted),))],
        compiler_params=params(8),
        name="pick_out",
    )(grad, *after)


def pair_sums(mine, other, zs, groups, after=()):
    m = len(zs)

    def body(g, o, *refs):
        own, *codes = refs[len(after) :]
        for d in (2, 1, 3, 0):
            for i, e in enumerate(zs):
                at = pl.ds((d * m + i) * W, W)
                total = g[:, at].astype(jnp.float32) + o[:, at].astype(jnp.float32)
                if d == 0:
                    own[:, i * W : (i + 1) * W] = total
                else:
                    q = [e in group for group in groups].index(True)
                    ref = codes[q * 3 + d - 1]
                    to = pl.ds(groups[q].index(e) * W, W)
                    code, scale = encode(total, PAIR_BOUND)
                    ref[0:W, to] = code
                    ref[W : W + EXTRA, to] = scale

    sent = [jax.ShapeDtypeStruct((W + EXTRA, len(group) * W), jnp.int16) for group in groups for _ in range(3)]
    return pl.pallas_call(
        body,
        out_shape=(jax.ShapeDtypeStruct((W, m * W), jnp.float32), *sent),
        in_specs=[VM, VM] + [ANY] * len(after),
        out_specs=(VM,) * (1 + len(sent)),
        compiler_params=params(12),
        name="pair_sums",
    )(mine, other, *after)


def octet_sums(own, got, after=()):
    m = got[0].shape[1] // W

    def body(own, g1, g2, g3, *refs):
        outs = refs[len(after) :]
        for i in range(m):
            at = pl.ds(i * W, W)
            total = own[:, at]
            for ref in (g1, g2, g3):
                total = total + decode(ref[0:W, at], ref[W : W + 1, at], PAIR_BOUND)
            code, scale = encode(total, OCTET_BOUND)
            outs[i][0:W, :] = code
            outs[i][W : W + EXTRA, :] = scale

    return pl.pallas_call(
        body,
        out_shape=(jax.ShapeDtypeStruct((W + EXTRA, W), jnp.int16),) * m,
        in_specs=[VM] * 4 + [ANY] * len(after),
        out_specs=(VM,) * m,
        compiler_params=params(12),
        name="octet_sums",
    )(own, *got, *after)


def dot(a, b, dims=((1,), (0,)), precision=None):
    return lax.dot_general(a, b, (dims, ((), ())), precision=precision, preferred_element_type=jnp.float32)


def thirds(value):
    first = value.astype(jnp.bfloat16)
    rest = value - first.astype(jnp.float32)
    second = rest.astype(jnp.bfloat16)
    third = (rest - second.astype(jnp.float32)).astype(jnp.bfloat16)
    return first, second, third


def own_masks(ids):
    lane = lax.broadcasted_iota(jnp.int32, (1, 512), 1)
    down = lax.broadcasted_iota(jnp.int32, (W, 512), 0)
    row = (lane >> 7) * BLOCK + (ids >> 6)
    col = ((lane >> 5) & 3) * BLOCK + (ids & 63)
    return down == row, down == col


def transform(own, along_x, along_z, momentum, table, ids):
    def body(own, x1, x2, x3, z1, z2, z3, mom, table, ids, acc_out, coeff_out, note_out):
        total = own[:, W : 2 * W]
        for ref in (x1, x2, x3):
            total = total + decode(ref[0:W, :], ref[W : W + 1, :], PAIR_BOUND)
        for ref in (z1, z2, z3):
            total = total + decode(ref[0:W, :], ref[W : W + 1, :], OCTET_BOUND)
        acc = DECAY * mom[...] + total
        acc_out[...] = acc
        t = table[...]
        coeffs = dot(dot(t, acc, precision=HI), t, ((1,), (1,)), HI)
        coeff_out[...] = coeffs
        rows, cols = own_masks(ids[...])
        chosen = cols.astype(jnp.float32).astype(jnp.bfloat16)
        parts = thirds(coeffs)
        spread = dot(parts[0], chosen) + (dot(parts[1], chosen) + dot(parts[2], chosen))
        note_out[:, 0:512] = jnp.sum(jnp.where(rows, spread, 0.0), axis=0, keepdims=True)
        note_out[:, 512:1024] = ids[...].astype(jnp.float32)

    return pl.pallas_call(
        body,
        out_shape=(
            jax.ShapeDtypeStruct((W, W), jnp.float32),
            jax.ShapeDtypeStruct((W, W), jnp.float32),
            jax.ShapeDtypeStruct((1, 1024), jnp.float32),
        ),
        in_specs=[VM] * 10,
        out_specs=(VM, VM, VM),
        compiler_params=params(16),
        name="transform",
    )(own, *along_x, *along_z, momentum, table, ids)


def momentum_step(acc, coeffs, table, ids):
    def body(acc, coeffs, table, ids, out):
        rows, cols = own_masks(ids[...])
        mask = dot(rows.astype(jnp.float32).astype(jnp.bfloat16), cols.astype(jnp.float32).astype(jnp.bfloat16), ((1,), (1,)))
        dense = jnp.where(mask > 0.5, coeffs[...], 0.0)
        t = table[...]
        out[...] = acc[...] - dot(dot(t, dense, ((0,), (0,)), HI), t, precision=HI)

    return pl.pallas_call(
        body,
        out_shape=jax.ShapeDtypeStruct((W, W), jnp.float32),
        in_specs=[VM] * 4,
        out_specs=VM,
        compiler_params=params(16),
        cost_estimate=pl.CostEstimate(flops=10**9, transcendentals=0, bytes_accessed=10**6),
        name="momentum_step",
    )(acc, coeffs, table, ids)


def bundle(parts, flat=False):
    shape = parts[0].shape
    out_shape = (len(parts),) + (shape[1:] if flat else shape)

    def body(*refs):
        out = refs[-1]
        for i in range(len(parts)):
            if flat:
                out[i : i + 1, :] = refs[i][...]
            else:
                out[i] = refs[i][...]

    return pl.pallas_call(
        body,
        out_shape=jax.ShapeDtypeStruct(out_shape, parts[0].dtype),
        in_specs=[VM] * len(parts),
        out_specs=VM,
        compiler_params=params(8),
        name="bundle",
    )(*parts)


def master_step(master, table, near, far):
    def body(master, table, near, far, out, low):
        me = lax.axis_index("group")
        notes = [near[i : i + 1, :] for i in range(4)] + [far[i : i + 1, :] for i in range(4)]
        ordered = []
        for g in range(8):
            rel = me ^ g
            found = notes[0]
            for r in range(1, 8):
                found = jnp.where(rel == r, notes[r], found)
            ordered.append(found)
        bands = []
        for a in range(4):
            v = jnp.concatenate([x[:, a * 128 : a * 128 + 128] for x in ordered], axis=1)
            k = jnp.concatenate([x[:, 512 + a * 128 : 640 + a * 128] for x in ordered], axis=1).astype(jnp.int32)
            lane = lax.broadcasted_iota(jnp.int32, (1, 1024), 1)
            row = lax.broadcasted_iota(jnp.int32, (BLOCK, 1024), 0) == (k >> 6)
            col = lax.broadcasted_iota(jnp.int32, (W, 1024), 0) == (((lane >> 5) & 3) * BLOCK + (k & 63))
            col = col.astype(jnp.float32).astype(jnp.bfloat16)
            stack = jnp.concatenate([jnp.where(row, p.astype(jnp.float32), 0.0).astype(jnp.bfloat16) for p in thirds(v)], axis=0)
            both = dot(stack, col, ((1,), (1,)))
            bands.append(both[0:BLOCK] + (both[BLOCK : 2 * BLOCK] + both[2 * BLOCK :]))
        union = jnp.concatenate(bands, axis=0)
        t = table[...]
        change = dot(dot(t, union, ((0,), (0,)), HI), t, precision=HI)
        result = master[...] - STEP * jnp.tanh(change)
        out[...] = result
        low[...] = result.astype(jnp.bfloat16)

    return pl.pallas_call(
        body,
        out_shape=(jax.ShapeDtypeStruct((W, W), jnp.float32), jax.ShapeDtypeStruct((W, W), jnp.bfloat16)),
        in_specs=[VM] * 4,
        out_specs=(VM, VM),
        compiler_params=params(16),
        name="master_step",
    )(master, table, near, far)


def joined(stacks, keys, whole=None):
    count = sum(len(k) for k in keys)

    def body(*refs):
        out, sem = refs[-2:]
        place = own_place()
        copies = []
        for ref, places in zip(refs, keys):
            for i, key in enumerate(places):
                source = ref.at[i] if len(places) > 1 else ref
                copy = pltpu.make_async_copy(source, out.at[:, pl.ds(column(*key, place), W)], sem.at[len(copies)])
                copy.start()
                copies.append(copy)
        for copy in copies:
            copy.wait()

    more = () if whole is None else (whole,)
    return pl.pallas_call(
        body,
        out_shape=jax.ShapeDtypeStruct((W, 32 * W), jnp.bfloat16),
        in_specs=[VM] * len(stacks) + [ANY] * len(more),
        out_specs=ANY,
        input_output_aliases={len(stacks): 0} if more else {},
        scratch_shapes=[pltpu.SemaphoreType.DMA((count,))],
        compiler_params=params(12),
        name="joined",
    )(*stacks, *more)


NEXT = (2, 1, 3)


def step(gradients, momentum, master, indices):
    table = jnp.asarray(cosine_blocks())
    grad = pltpu.with_memory_space_constraint(gradients[0, 0], pltpu.HBM)
    ids = indices[0].reshape(1, 512)

    far, near = (2, 3), (1, 0)
    (given_far,) = pick_out(grad, ((far, 1),))
    mine_far, given_near, mine_near = pick_out(grad, ((far, 0), (near, 1), (near, 0)), (given_far,))
    own_far, *codes_far = pair_sums(mine_far, swapped(given_far, "c", 1), far, (far,))
    got_far = {d: swapped(codes_far[d - 1], "x", d) for d in NEXT}
    own_near, *codes_near = pair_sums(mine_near, swapped(given_near, "c", 1), near, ((1,), (0,)), (own_far,))
    got_mid = {d: swapped(codes_near[d - 1], "x", d) for d in NEXT}
    got_own = {d: swapped(codes_near[d + 2], "x", d) for d in NEXT}
    out2, out3 = octet_sums(own_far, [got_far[d] for d in (1, 2, 3)])
    in2, in3 = swapped(out2, "z", 2), swapped(out3, "z", 3)
    (out1,) = octet_sums(own_near, [got_mid[d] for d in (1, 2, 3)], (out2,))
    in1 = swapped(out1, "z", 1)

    acc, coeffs, note = transform(own_near, [got_own[d] for d in (1, 2, 3)], (in1, in2, in3), momentum[0], table, ids)
    notes = [note] + [swapped(note, "group", r) for r in (1, 2, 3)]
    momentum_out = momentum_step(acc, coeffs, table, ids)
    mine = bundle(notes, flat=True)
    theirs = swapped(mine, "group", 4)
    master_out, low = master_step(master, table, mine, theirs)

    by_z = [low] + [swapped(low, "z", e) for e in (1, 2, 3)]
    by_x = {(d, e): swapped(by_z[e], "x", d) for e in range(4) for d in NEXT}
    parts = {
        "early": [(0, e) for e in range(4)] + [(d, e) for e in (0, 1) for d in NEXT],
        "mid": [(d, 2) for d in NEXT],
        "late": [(d, 3) for d in NEXT],
    }
    by_x.update({(0, e): by_z[e] for e in range(4)})
    whole = None
    for keys in parts.values():
        half = bundle([by_x[key] for key in keys])
        other = swapped(half, "c", 1)
        whole = joined([half, other], [[(*key, f) for key in keys] for f in (0, 1)], whole)
    params_full = whole
    return momentum_out[None], master_out, params_full


def solution(mesh):
    torus = Mesh(mesh.devices.reshape(mesh.shape["group"], 4, 4, 2), ("group", "x", "z", "c"))
    return jax.shard_map(
        step,
        mesh=torus,
        in_specs=(P("group", SHARD, None, None), P("group", None, SHARD), P(None, SHARD), P("group", None, SHARD, None)),
        out_specs=(P("group", None, SHARD), P(None, SHARD), P()),
        check_vma=False,
    )
```

```python
import jax
import jax.numpy as jnp
import numpy as np
from jax import lax
from jax.experimental import pallas as pl
from jax.experimental.pallas import tpu as pltpu
from jax.sharding import Mesh
from jax.sharding import PartitionSpec as P


BLOCK = 64
W = 256
SHARD = ("x", "z", "c")
DECAY = 0.9
STEP = 0.5
TOP = 32767.0
EXTRA = 8
PAIR_BOUND = 3.2
OCTET_BOUND = 12.8
HI = lax.Precision.HIGHEST


def cosine_blocks():
    k = np.arange(BLOCK, dtype=np.float64)[:, None]
    n = np.arange(BLOCK, dtype=np.float64)[None, :]
    table = np.cos(np.pi * (2 * n + 1) * k / (2 * BLOCK)) * np.where(k == 0, np.sqrt(1 / BLOCK), np.sqrt(2 / BLOCK))
    return np.kron(np.eye(W // BLOCK), table).astype(np.float32)


def swapped(value, axis, mask):
    size = lax.axis_size(axis)
    return lax.ppermute(value, axis, [(i, i ^ mask) for i in range(size)])


def encode(field, bound):
    top = jnp.max(jnp.abs(field), axis=0, keepdims=True)
    scale = jnp.clip(jnp.ceil(top * (TOP / bound)), 1.0, TOP)
    code = jnp.round(field * ((TOP * TOP / bound) / scale))
    return code.astype(jnp.int32).astype(jnp.int16), jnp.broadcast_to(scale, (EXTRA, field.shape[1])).astype(jnp.int32).astype(jnp.int16)


def decode(code, scale, bound):
    return code.astype(jnp.int32).astype(jnp.float32) * (scale.astype(jnp.int32).astype(jnp.float32) * (bound / (TOP * TOP)))


ANY = pl.BlockSpec(memory_space=pl.ANY)
VM = pl.BlockSpec(memory_space=pltpu.VMEM)
HB = pl.BlockSpec(memory_space=pltpu.HBM)
MIB = 1 << 20


def params(mib):
    return pltpu.CompilerParams(vmem_limit_bytes=mib * MIB)


def own_place():
    return [lax.axis_index(name) for name in ("x", "z", "c")]


def column(d, e, flip, place):
    return pl.multiple_of((((place[0] ^ d) * 4 + (place[1] ^ e)) * 2 + (place[2] ^ flip)) * W, W)


def pick_out(grad, wanted, after=()):
    def body(g, *refs):
        outs, sem = refs[len(after) : -1], refs[-1]
        place = own_place()
        copies = []
        for out, (zs, flip) in zip(outs, wanted):
            for d in range(4):
                for i, e in enumerate(zs):
                    to = pl.ds((d * len(zs) + i) * W, W)
                    copy = pltpu.make_async_copy(g.at[:, pl.ds(column(d, e, flip, place), W)], out.at[:, to], sem.at[len(copies)])
                    copy.start()
                    copies.append(copy)
        for copy in copies:
            copy.wait()

    return pl.pallas_call(
        body,
        out_shape=tuple(jax.ShapeDtypeStruct((W, 4 * len(zs) * W), jnp.bfloat16) for zs, _ in wanted),
        in_specs=[HB] + [ANY] * len(after),
        out_specs=(VM,) * len(wanted),
        scratch_shapes=[pltpu.SemaphoreType.DMA((4 * sum(len(zs) for zs, _ in wanted),))],
        compiler_params=params(12),
        name="pick_out",
    )(grad, *after)


def pair_sums(mine, other, zs, after=()):
    m = len(zs)

    def body(g, o, *refs):
        own, *codes = refs[len(after) :]
        for d in (2, 1, 3, 0):
            for i in range(m):
                at = pl.ds((d * m + i) * W, W)
                total = g[:, at].astype(jnp.float32) + o[:, at].astype(jnp.float32)
                if d == 0:
                    own[:, i * W : (i + 1) * W] = total
                else:
                    ref = codes[i * 3 + d - 1]
                    code, scale = encode(total, PAIR_BOUND)
                    ref[0:W, :] = code
                    ref[W : W + EXTRA, :] = scale

    sent = [jax.ShapeDtypeStruct((W + EXTRA, W), jnp.int16)] * (3 * m)
    return pl.pallas_call(
        body,
        out_shape=(jax.ShapeDtypeStruct((W, m * W), jnp.float32), *sent),
        in_specs=[VM, VM] + [ANY] * len(after),
        out_specs=(VM,) * (1 + len(sent)),
        compiler_params=params(12),
        name="pair_sums",
    )(mine, other, *after)


def octet_sums(own, first, got, after=()):
    def body(own, g1, g2, g3, *refs):
        out = refs[-1]
        total = own[:, first : first + W]
        for ref in (g1, g2, g3):
            total = total + decode(ref[0:W, :], ref[W : W + 1, :], PAIR_BOUND)
        code, scale = encode(total, OCTET_BOUND)
        out[0:W, :] = code
        out[W : W + EXTRA, :] = scale

    return pl.pallas_call(
        body,
        out_shape=jax.ShapeDtypeStruct((W + EXTRA, W), jnp.int16),
        in_specs=[VM] * 4 + [ANY] * len(after),
        out_specs=VM,
        compiler_params=params(12),
        name="octet_sums",
    )(own, *got, *after)


def dot(a, b, dims=((1,), (0,)), precision=None):
    return lax.dot_general(a, b, (dims, ((), ())), precision=precision, preferred_element_type=jnp.float32)


def thirds(value):
    first = value.astype(jnp.bfloat16)
    rest = value - first.astype(jnp.float32)
    second = rest.astype(jnp.bfloat16)
    third = (rest - second.astype(jnp.float32)).astype(jnp.bfloat16)
    return first, second, third


def own_masks(ids):
    lane = lax.broadcasted_iota(jnp.int32, (1, 512), 1)
    down = lax.broadcasted_iota(jnp.int32, (W, 512), 0)
    row = (lane >> 7) * BLOCK + (ids >> 6)
    col = ((lane >> 5) & 3) * BLOCK + (ids & 63)
    return down == row, down == col


def transform(own, along_x, along_z, momentum, table, ids):
    def body(own, x1, x2, x3, z1, z2, z3, mom, table, ids, acc_out, coeff_out, note_out):
        total = own[:, 2 * W : 3 * W]
        for ref in (x1, x2, x3):
            total = total + decode(ref[0:W, :], ref[W : W + 1, :], PAIR_BOUND)
        for ref in (z1, z2, z3):
            total = total + decode(ref[0:W, :], ref[W : W + 1, :], OCTET_BOUND)
        acc = DECAY * mom[...] + total
        acc_out[...] = acc
        t = table[...]
        coeffs = dot(dot(t, acc, precision=HI), t, ((1,), (1,)), HI)
        coeff_out[...] = coeffs
        rows, cols = own_masks(ids[...])
        chosen = cols.astype(jnp.float32).astype(jnp.bfloat16)
        parts = thirds(coeffs)
        spread = dot(parts[0], chosen) + (dot(parts[1], chosen) + dot(parts[2], chosen))
        note_out[:, 0:512] = jnp.sum(jnp.where(rows, spread, 0.0), axis=0, keepdims=True)
        note_out[:, 512:1024] = ids[...].astype(jnp.float32)

    return pl.pallas_call(
        body,
        out_shape=(
            jax.ShapeDtypeStruct((W, W), jnp.float32),
            jax.ShapeDtypeStruct((W, W), jnp.float32),
            jax.ShapeDtypeStruct((1, 1024), jnp.float32),
        ),
        in_specs=[VM] * 10,
        out_specs=(VM, VM, VM),
        compiler_params=params(16),
        name="transform",
    )(own, *along_x, *along_z, momentum, table, ids)


def momentum_step(acc, coeffs, table, ids):
    def body(acc, coeffs, table, ids, out):
        rows, cols = own_masks(ids[...])
        mask = dot(rows.astype(jnp.float32).astype(jnp.bfloat16), cols.astype(jnp.float32).astype(jnp.bfloat16), ((1,), (1,)))
        dense = jnp.where(mask > 0.5, coeffs[...], 0.0)
        t = table[...]
        out[...] = acc[...] - dot(dot(t, dense, ((0,), (0,)), HI), t, precision=HI)

    return pl.pallas_call(
        body,
        out_shape=jax.ShapeDtypeStruct((W, W), jnp.float32),
        in_specs=[VM] * 4,
        out_specs=VM,
        compiler_params=params(16),
        cost_estimate=pl.CostEstimate(flops=10**9, transcendentals=0, bytes_accessed=10**6),
        name="momentum_step",
    )(acc, coeffs, table, ids)


def bundle(parts, flat=False):
    shape = parts[0].shape
    out_shape = (len(parts),) + (shape[1:] if flat else shape)

    def body(*refs):
        out = refs[-1]
        for i in range(len(parts)):
            if flat:
                out[i : i + 1, :] = refs[i][...]
            else:
                out[i] = refs[i][...]

    return pl.pallas_call(
        body,
        out_shape=jax.ShapeDtypeStruct(out_shape, parts[0].dtype),
        in_specs=[VM] * len(parts),
        out_specs=VM,
        compiler_params=params(8),
        name="bundle",
    )(*parts)


def master_step(master, table, near, far):
    def body(master, table, near, far, out, low):
        me = lax.axis_index("group")
        notes = [near[i : i + 1, :] for i in range(4)] + [far[i : i + 1, :] for i in range(4)]
        ordered = []
        for g in range(8):
            rel = me ^ g
            found = notes[0]
            for r in range(1, 8):
                found = jnp.where(rel == r, notes[r], found)
            ordered.append(found)
        bands = []
        for a in range(4):
            v = jnp.concatenate([x[:, a * 128 : a * 128 + 128] for x in ordered], axis=1)
            k = jnp.concatenate([x[:, 512 + a * 128 : 640 + a * 128] for x in ordered], axis=1).astype(jnp.int32)
            lane = lax.broadcasted_iota(jnp.int32, (1, 1024), 1)
            row = lax.broadcasted_iota(jnp.int32, (BLOCK, 1024), 0) == (k >> 6)
            col = lax.broadcasted_iota(jnp.int32, (W, 1024), 0) == (((lane >> 5) & 3) * BLOCK + (k & 63))
            col = col.astype(jnp.float32).astype(jnp.bfloat16)
            stack = jnp.concatenate([jnp.where(row, p.astype(jnp.float32), 0.0).astype(jnp.bfloat16) for p in thirds(v)], axis=0)
            both = dot(stack, col, ((1,), (1,)))
            bands.append(both[0:BLOCK] + (both[BLOCK : 2 * BLOCK] + both[2 * BLOCK :]))
        union = jnp.concatenate(bands, axis=0)
        t = table[...]
        change = dot(dot(t, union, ((0,), (0,)), HI), t, precision=HI)
        result = master[...] - STEP * jnp.tanh(change)
        out[...] = result
        low[...] = result.astype(jnp.bfloat16)

    return pl.pallas_call(
        body,
        out_shape=(jax.ShapeDtypeStruct((W, W), jnp.float32), jax.ShapeDtypeStruct((W, W), jnp.bfloat16)),
        in_specs=[VM] * 4,
        out_specs=(VM, VM),
        compiler_params=params(16),
        name="master_step",
    )(master, table, near, far)


def joined(stacks, keys, whole=None):
    count = sum(len(k) for k in keys)

    def body(*refs):
        out, sem = refs[-2:]
        place = own_place()
        copies = []
        for ref, places in zip(refs, keys):
            for i, key in enumerate(places):
                source = ref.at[i] if len(places) > 1 else ref
                copy = pltpu.make_async_copy(source, out.at[:, pl.ds(column(*key, place), W)], sem.at[len(copies)])
                copy.start()
                copies.append(copy)
        for copy in copies:
            copy.wait()

    more = () if whole is None else (whole,)
    return pl.pallas_call(
        body,
        out_shape=jax.ShapeDtypeStruct((W, 32 * W), jnp.bfloat16),
        in_specs=[VM] * len(stacks) + [ANY] * len(more),
        out_specs=ANY,
        input_output_aliases={len(stacks): 0} if more else {},
        scratch_shapes=[pltpu.SemaphoreType.DMA((count,))],
        compiler_params=params(12),
        name="joined",
    )(*stacks, *more)


NEXT = (2, 1, 3)


def step(gradients, momentum, master, indices):
    table = jnp.asarray(cosine_blocks())
    grad = pltpu.with_memory_space_constraint(gradients[0, 0], pltpu.HBM)
    ids = indices[0].reshape(1, 512)

    far, near = (2,), (3, 1, 0)
    (given_far,) = pick_out(grad, ((far, 1),))
    mine_far, given_near, mine_near = pick_out(grad, ((far, 0), (near, 1), (near, 0)), (given_far,))
    own_far, *codes_far = pair_sums(mine_far, swapped(given_far, "c", 1), far)
    own_near, *codes_near = pair_sums(mine_near, swapped(given_near, "c", 1), near, (own_far,))
    codes = {e: part[i * 3 : i * 3 + 3] for part, zs in ((codes_far, far), (codes_near, near)) for i, e in enumerate(zs)}
    got = {e: [swapped(codes[e][d - 1], "x", d) for d in (1, 2, 3)] for e in (2, 3, 1, 0)}
    out2 = octet_sums(own_far, 0, got[2])
    out3 = octet_sums(own_near, 0, got[3], (out2,))
    out1 = octet_sums(own_near, W, got[1], (out3,))
    in2, in3, in1 = (swapped(out, "z", e) for e, out in ((2, out2), (3, out3), (1, out1)))

    acc, coeffs, note = transform(own_near, got[0], (in1, in2, in3), momentum[0], table, ids)
    notes = [note] + [swapped(note, "group", r) for r in (1, 2, 3)]
    momentum_out = momentum_step(acc, coeffs, table, ids)
    mine = bundle(notes, flat=True)
    theirs = swapped(mine, "group", 4)
    master_out, low = master_step(master, table, mine, theirs)

    by_z = [low] + [swapped(low, "z", e) for e in (1, 2, 3)]
    by_x = {(d, e): swapped(by_z[e], "x", d) for e in range(4) for d in NEXT}
    parts = {
        "early": [(0, e) for e in range(4)] + [(d, e) for e in (0, 1) for d in NEXT],
        "mid": [(d, 2) for d in NEXT],
        "late": [(d, 3) for d in NEXT],
    }
    by_x.update({(0, e): by_z[e] for e in range(4)})
    whole = None
    for keys in parts.values():
        half = bundle([by_x[key] for key in keys])
        other = swapped(half, "c", 1)
        whole = joined([half, other], [[(*key, f) for key in keys] for f in (0, 1)], whole)
    params_full = whole
    return momentum_out[None], master_out, params_full


def solution(mesh):
    torus = Mesh(mesh.devices.reshape(mesh.shape["group"], 4, 4, 2), ("group", "x", "z", "c"))
    return jax.shard_map(
        step,
        mesh=torus,
        in_specs=(P("group", SHARD, None, None), P("group", None, SHARD), P(None, SHARD), P("group", None, SHARD, None)),
        out_specs=(P("group", None, SHARD), P(None, SHARD), P()),
        check_vma=False,
    )
```

```python
import jax
import jax.numpy as jnp
import numpy as np
from jax import lax
from jax.experimental import pallas as pl
from jax.experimental.pallas import tpu as pltpu
from jax.sharding import Mesh
from jax.sharding import PartitionSpec as P


BLOCK = 64
W = 256
SHARD = ("x", "z", "c")
DECAY = 0.9
STEP = 0.5
TOP = 32767.0
EXTRA = 8
PAIR_BOUND = 3.2
OCTET_BOUND = 12.8
HI = lax.Precision.HIGHEST


def cosine_blocks():
    k = np.arange(BLOCK, dtype=np.float64)[:, None]
    n = np.arange(BLOCK, dtype=np.float64)[None, :]
    table = np.cos(np.pi * (2 * n + 1) * k / (2 * BLOCK)) * np.where(k == 0, np.sqrt(1 / BLOCK), np.sqrt(2 / BLOCK))
    return np.kron(np.eye(W // BLOCK), table).astype(np.float32)


def swapped(value, axis, mask):
    size = lax.axis_size(axis)
    return lax.ppermute(value, axis, [(i, i ^ mask) for i in range(size)])


def encode(field, bound):
    top = jnp.max(jnp.abs(field), axis=0, keepdims=True)
    scale = jnp.clip(jnp.ceil(top * (TOP / bound)), 1.0, TOP)
    code = jnp.round(field * ((TOP * TOP / bound) / scale))
    return code.astype(jnp.int32).astype(jnp.int16), jnp.broadcast_to(scale, (EXTRA, field.shape[1])).astype(jnp.int32).astype(jnp.int16)


def decode(code, scale, bound):
    return code.astype(jnp.int32).astype(jnp.float32) * (scale.astype(jnp.int32).astype(jnp.float32) * (bound / (TOP * TOP)))


ANY = pl.BlockSpec(memory_space=pl.ANY)
VM = pl.BlockSpec(memory_space=pltpu.VMEM)
HB = pl.BlockSpec(memory_space=pltpu.HBM)
MIB = 1 << 20


def params(mib):
    return pltpu.CompilerParams(vmem_limit_bytes=mib * MIB)


def own_place():
    return [lax.axis_index(name) for name in ("x", "z", "c")]


def column(d, e, flip, place):
    return pl.multiple_of((((place[0] ^ d) * 4 + (place[1] ^ e)) * 2 + (place[2] ^ flip)) * W, W)


def pick_out(grad, wanted, after=()):
    def body(g, *refs):
        outs, sem = refs[len(after) : -1], refs[-1]
        place = own_place()
        copies = []
        for out, (zs, flip) in zip(outs, wanted):
            for d in range(4):
                for i, e in enumerate(zs):
                    to = pl.ds((d * len(zs) + i) * W, W)
                    copy = pltpu.make_async_copy(g.at[:, pl.ds(column(d, e, flip, place), W)], out.at[:, to], sem.at[len(copies)])
                    copy.start()
                    copies.append(copy)
        for copy in copies:
            copy.wait()

    return pl.pallas_call(
        body,
        out_shape=tuple(jax.ShapeDtypeStruct((W, 4 * len(zs) * W), jnp.bfloat16) for zs, _ in wanted),
        in_specs=[HB] + [ANY] * len(after),
        out_specs=(VM,) * len(wanted),
        scratch_shapes=[pltpu.SemaphoreType.DMA((4 * sum(len(zs) for zs, _ in wanted),))],
        compiler_params=params(12),
        name="pick_out",
    )(grad, *after)


def pair_sums(mine, other, zs, after=()):
    m = len(zs)

    def body(g, o, *refs):
        own, *codes = refs[len(after) :]
        for d in (2, 1, 3, 0):
            for i in range(m):
                at = pl.ds((d * m + i) * W, W)
                total = g[:, at].astype(jnp.float32) + o[:, at].astype(jnp.float32)
                if d == 0:
                    own[:, i * W : (i + 1) * W] = total
                else:
                    ref = codes[i * 3 + d - 1]
                    code, scale = encode(total, PAIR_BOUND)
                    ref[0:W, :] = code
                    ref[W : W + EXTRA, :] = scale

    sent = [jax.ShapeDtypeStruct((W + EXTRA, W), jnp.int16)] * (3 * m)
    return pl.pallas_call(
        body,
        out_shape=(jax.ShapeDtypeStruct((W, m * W), jnp.float32), *sent),
        in_specs=[VM, VM] + [ANY] * len(after),
        out_specs=(VM,) * (1 + len(sent)),
        compiler_params=params(12),
        name="pair_sums",
    )(mine, other, *after)


def octet_sums(own, first, got, after=()):
    def body(own, g1, g2, g3, *refs):
        out = refs[-1]
        total = own[:, first : first + W]
        for ref in (g1, g2, g3):
            total = total + decode(ref[0:W, :], ref[W : W + 1, :], PAIR_BOUND)
        code, scale = encode(total, OCTET_BOUND)
        out[0:W, :] = code
        out[W : W + EXTRA, :] = scale

    return pl.pallas_call(
        body,
        out_shape=jax.ShapeDtypeStruct((W + EXTRA, W), jnp.int16),
        in_specs=[VM] * 4 + [ANY] * len(after),
        out_specs=VM,
        compiler_params=params(12),
        name="octet_sums",
    )(own, *got, *after)


def dot(a, b, dims=((1,), (0,)), precision=None):
    return lax.dot_general(a, b, (dims, ((), ())), precision=precision, preferred_element_type=jnp.float32)


def thirds(value):
    first = value.astype(jnp.bfloat16)
    rest = value - first.astype(jnp.float32)
    second = rest.astype(jnp.bfloat16)
    third = (rest - second.astype(jnp.float32)).astype(jnp.bfloat16)
    return first, second, third


def own_masks(ids):
    lane = lax.broadcasted_iota(jnp.int32, (1, 512), 1)
    down = lax.broadcasted_iota(jnp.int32, (W, 512), 0)
    row = (lane >> 7) * BLOCK + (ids >> 6)
    col = ((lane >> 5) & 3) * BLOCK + (ids & 63)
    return down == row, down == col


def transform(own, along_x, along_z, momentum, table, ids):
    def body(own, x1, x2, x3, z1, z2, z3, mom, table, ids, acc_out, coeff_out, note_out):
        total = own[:, 2 * W : 3 * W]
        for ref in (x1, x2, x3):
            total = total + decode(ref[0:W, :], ref[W : W + 1, :], PAIR_BOUND)
        for ref in (z1, z2, z3):
            total = total + decode(ref[0:W, :], ref[W : W + 1, :], OCTET_BOUND)
        acc = DECAY * mom[...] + total
        acc_out[...] = acc
        t = table[...]
        coeffs = dot(dot(t, acc, precision=HI), t, ((1,), (1,)), HI)
        coeff_out[...] = coeffs
        rows, cols = own_masks(ids[...])
        chosen = cols.astype(jnp.float32).astype(jnp.bfloat16)
        parts = thirds(coeffs)
        spread = dot(parts[0], chosen) + (dot(parts[1], chosen) + dot(parts[2], chosen))
        note_out[:, 0:512] = jnp.sum(jnp.where(rows, spread, 0.0), axis=0, keepdims=True)
        note_out[:, 512:1024] = ids[...].astype(jnp.float32)

    return pl.pallas_call(
        body,
        out_shape=(
            jax.ShapeDtypeStruct((W, W), jnp.float32),
            jax.ShapeDtypeStruct((W, W), jnp.float32),
            jax.ShapeDtypeStruct((1, 1024), jnp.float32),
        ),
        in_specs=[VM] * 10,
        out_specs=(VM, VM, VM),
        compiler_params=params(16),
        name="transform",
    )(own, *along_x, *along_z, momentum, table, ids)


def momentum_step(acc, coeffs, table, ids):
    def body(acc, coeffs, table, ids, out):
        rows, cols = own_masks(ids[...])
        mask = dot(rows.astype(jnp.float32).astype(jnp.bfloat16), cols.astype(jnp.float32).astype(jnp.bfloat16), ((1,), (1,)))
        dense = jnp.where(mask > 0.5, coeffs[...], 0.0)
        t = table[...]
        out[...] = acc[...] - dot(dot(t, dense, ((0,), (0,)), HI), t, precision=HI)

    return pl.pallas_call(
        body,
        out_shape=jax.ShapeDtypeStruct((W, W), jnp.float32),
        in_specs=[VM] * 4,
        out_specs=VM,
        compiler_params=params(16),
        cost_estimate=pl.CostEstimate(flops=10**9, transcendentals=0, bytes_accessed=10**6),
        name="momentum_step",
    )(acc, coeffs, table, ids)


def bundle(parts, flat=False):
    shape = parts[0].shape
    out_shape = (len(parts),) + (shape[1:] if flat else shape)

    def body(*refs):
        out = refs[-1]
        for i in range(len(parts)):
            if flat:
                out[i : i + 1, :] = refs[i][...]
            else:
                out[i] = refs[i][...]

    return pl.pallas_call(
        body,
        out_shape=jax.ShapeDtypeStruct(out_shape, parts[0].dtype),
        in_specs=[VM] * len(parts),
        out_specs=VM,
        compiler_params=params(8),
        name="bundle",
    )(*parts)


def union_of(notes, me):
    rows = [notes[r : r + 1, :] for r in range(4)]
    ordered = []
    for q in range(4):
        rel = (me & 3) ^ q
        found = rows[0]
        for r in range(1, 4):
            found = jnp.where(rel == r, rows[r], found)
        ordered.append(found)
    bands = []
    for a in range(4):
        v = jnp.concatenate([x[:, a * 128 : a * 128 + 128] for x in ordered], axis=1)
        k = jnp.concatenate([x[:, 512 + a * 128 : 640 + a * 128] for x in ordered], axis=1).astype(jnp.int32)
        lane = lax.broadcasted_iota(jnp.int32, (1, 512), 1)
        row = lax.broadcasted_iota(jnp.int32, (BLOCK, 512), 0) == (k >> 6)
        col = lax.broadcasted_iota(jnp.int32, (W, 512), 0) == (((lane >> 5) & 3) * BLOCK + (k & 63))
        col = col.astype(jnp.float32).astype(jnp.bfloat16)
        stack = jnp.concatenate([jnp.where(row, p.astype(jnp.float32), 0.0).astype(jnp.bfloat16) for p in thirds(v)], axis=0)
        both = dot(stack, col, ((1,), (1,)))
        bands.append(both[0:BLOCK] + (both[BLOCK : 2 * BLOCK] + both[2 * BLOCK :]))
    return jnp.concatenate(bands, axis=0)


def near_union(notes):
    def body(notes, out):
        out[...] = union_of(notes, lax.axis_index("group"))

    return pl.pallas_call(
        body,
        out_shape=jax.ShapeDtypeStruct((W, W), jnp.float32),
        in_specs=[VM],
        out_specs=VM,
        compiler_params=params(16),
        name="near_union",
    )(notes)


def master_step(master, table, near, far):
    def body(master, table, near, far, out, low):
        union = near[...] + union_of(far, lax.axis_index("group"))
        t = table[...]
        change = dot(dot(t, union, ((0,), (0,)), HI), t, precision=HI)
        result = master[...] - STEP * jnp.tanh(change)
        out[...] = result
        low[...] = result.astype(jnp.bfloat16)

    return pl.pallas_call(
        body,
        out_shape=(jax.ShapeDtypeStruct((W, W), jnp.float32), jax.ShapeDtypeStruct((W, W), jnp.bfloat16)),
        in_specs=[VM] * 4,
        out_specs=(VM, VM),
        compiler_params=params(16),
        name="master_step",
    )(master, table, near, far)


def joined(stacks, keys, whole=None):
    count = sum(len(k) for k in keys)

    def body(*refs):
        out, sem = refs[-2:]
        place = own_place()
        copies = []
        for ref, places in zip(refs, keys):
            for i, key in enumerate(places):
                source = ref.at[i] if len(places) > 1 else ref
                copy = pltpu.make_async_copy(source, out.at[:, pl.ds(column(*key, place), W)], sem.at[len(copies)])
                copy.start()
                copies.append(copy)
        for copy in copies:
            copy.wait()

    more = () if whole is None else (whole,)
    return pl.pallas_call(
        body,
        out_shape=jax.ShapeDtypeStruct((W, 32 * W), jnp.bfloat16),
        in_specs=[VM] * len(stacks) + [ANY] * len(more),
        out_specs=ANY,
        input_output_aliases={len(stacks): 0} if more else {},
        scratch_shapes=[pltpu.SemaphoreType.DMA((count,))],
        compiler_params=params(12),
        name="joined",
    )(*stacks, *more)


NEXT = (2, 1, 3)


def step(gradients, momentum, master, indices):
    table = jnp.asarray(cosine_blocks())
    grad = pltpu.with_memory_space_constraint(gradients[0, 0], pltpu.HBM)
    ids = indices[0].reshape(1, 512)

    far, near = (2,), (3, 1, 0)
    (given_far,) = pick_out(grad, ((far, 1),))
    mine_far, given_near, mine_near = pick_out(grad, ((far, 0), (near, 1), (near, 0)), (given_far,))
    own_far, *codes_far = pair_sums(mine_far, swapped(given_far, "c", 1), far)
    own_near, *codes_near = pair_sums(mine_near, swapped(given_near, "c", 1), near, (own_far,))
    codes = {e: part[i * 3 : i * 3 + 3] for part, zs in ((codes_far, far), (codes_near, near)) for i, e in enumerate(zs)}
    got = {e: [swapped(codes[e][d - 1], "x", d) for d in (1, 2, 3)] for e in (2, 3, 1, 0)}
    out2 = octet_sums(own_far, 0, got[2])
    out3 = octet_sums(own_near, 0, got[3], (out2,))
    out1 = octet_sums(own_near, W, got[1], (out3,))
    in2, in3, in1 = (swapped(out, "z", e) for e, out in ((2, out2), (3, out3), (1, out1)))

    acc, coeffs, note = transform(own_near, got[0], (in1, in2, in3), momentum[0], table, ids)
    notes = [note] + [swapped(note, "group", r) for r in (1, 2, 3)]
    momentum_out = momentum_step(acc, coeffs, table, ids)
    mine = bundle(notes, flat=True)
    theirs = swapped(mine, "group", 4)
    partly = near_union(mine)
    master_out, low = master_step(master, table, partly, theirs)

    by_z = [low] + [swapped(low, "z", e) for e in (1, 2, 3)]
    by_x = {(d, e): swapped(by_z[e], "x", d) for e in range(4) for d in NEXT}
    parts = {
        "early": [(0, e) for e in range(4)] + [(d, e) for e in (0, 1) for d in NEXT],
        "mid": [(d, 2) for d in NEXT],
        "late": [(d, 3) for d in NEXT],
    }
    by_x.update({(0, e): by_z[e] for e in range(4)})
    whole = None
    for keys in parts.values():
        half = bundle([by_x[key] for key in keys])
        other = swapped(half, "c", 1)
        whole = joined([half, other], [[(*key, f) for key in keys] for f in (0, 1)], whole)
    params_full = whole
    return momentum_out[None], master_out, params_full


def solution(mesh):
    torus = Mesh(mesh.devices.reshape(mesh.shape["group"], 4, 4, 2), ("group", "x", "z", "c"))
    return jax.shard_map(
        step,
        mesh=torus,
        in_specs=(P("group", SHARD, None, None), P("group", None, SHARD), P(None, SHARD), P("group", None, SHARD, None)),
        out_specs=(P("group", None, SHARD), P(None, SHARD), P()),
        check_vma=False,
    )
```
